32 devices in a mesh: dp: 8 (over z, x), feat: 4 (over y, core).
Axes of the slice: x: 2, y: 2, z: 4, core: 2. Of those that a mesh axis runs over, the one named last changes fastest.
Arguments:
- activations: bfloat16 [2048, 8192], P('dp', 'feat'), may hold values from -6 to 6
- cotangent: bfloat16 [2048, 1024], P('dp'), may hold values from -0.13183594 to 0.13183594
- weight: float32 [8192, 1024], P('feat'), may hold values from -0.0625 to 0.0625
- stats_old: float32 [4, 8, 4, 256, 256], P('feat', 'dp'), as said below
- owners: int32 [32, 4], replicated, may hold values from 0 to 7, as said below
- next_acts: bfloat16 [2048, 8192], P('dp', 'feat'), may hold values from -6 to 6
Outputs:
- weight_new: float32 [8192, 1024], P('feat')
- stats_new: float32 [4, 8, 4, 256, 256], P('feat', 'dp')
- next_out: bfloat16 [2048, 1024], P('dp', 'feat')
The draws below stay inside these ranges and needn't reach their ends.
Inputs may be any that keep to these rules, and one draw needn't show every extreme that they name: `owners`: blocks are grouped by the index of feat that holds their rows (8192 / (256 * 4) row blocks a group); in every group each dp index owns at most 4 blocks, and some dp index owns exactly 4. `stats_old`: every slot holds a symmetric positive definite matrix; slots that no block maps to are not read.
All inputs are finite; a program needn't handle non-finite values.
Results may differ from the reference program's by a relative error of at most 0.02.
Values may be sent and summed in bfloat16 or wider, within the bound.
A program may use at most 128 MiB of HBM per device.

```python
import jax
import jax.numpy as jnp
from jax import lax

D = 8192
COLS = 1024
BLOCK = 256
ITERS = 6
TOKENS = 2048
MOST = 4
N_DP = 8
N_FEAT = 4


def draw_owners(key, part):
    block_count = D // (BLOCK * N_FEAT) * (COLS // BLOCK)
    group_keys = jax.random.split(jax.random.fold_in(key, 11), N_FEAT)
    order_keys = jax.random.split(jax.random.fold_in(key, 23), N_FEAT)
    chosen = jax.vmap(lambda sub: jax.random.permutation(sub, N_DP))(group_keys).astype(jnp.int32)
    place_ids = jnp.arange(block_count, dtype=jnp.int32)
    pick_ids = jnp.where(place_ids < MOST, 0, 1 + jnp.maximum(place_ids - MOST, 0) % (N_DP - 1)).astype(jnp.int32)
    listing = chosen[:, pick_ids]
    shuffle = jax.vmap(lambda sub: jax.random.permutation(sub, block_count))(order_keys).astype(jnp.int32)
    placed = jnp.take_along_axis(listing, shuffle, axis=1)
    return placed.reshape(D // BLOCK, COLS // BLOCK).astype(jnp.int32)


def draw_stats_old(key, part):
    shape = (N_FEAT, N_DP, MOST, BLOCK, BLOCK)
    base = jax.random.normal(jax.random.fold_in(key, 31), shape, jnp.float32)
    product = jnp.einsum('abcij,abckj->abcik', base, base, precision=lax.Precision.HIGHEST) / BLOCK
    identity = jnp.eye(BLOCK, dtype=jnp.float32)
    return (product + 0.125 * identity).astype(jnp.float32)


def block_scale(key, dims, shards, smallest, high):
    factor_of = 1.0
    for dim, blocks in shards:
        draws = jax.random.uniform(jax.random.fold_in(jax.random.fold_in(key, 6), dim), (blocks,), jnp.float32, smallest / len(shards), high / len(shards))
        factor_of = factor_of * jnp.repeat(jnp.exp(draws), dims[dim] // blocks).reshape((-1,) + (1,) * (len(dims) - 1 - dim))
    return factor_of


def noise(own_key, dims, spread, limit, cuts=(), kind=jnp.bfloat16):
    result = spread * jax.random.normal(own_key, dims, jnp.float32)
    if cuts:
        result = result * block_scale(own_key, dims, cuts, -0.22, 0.18)
    return jnp.clip(result, -limit, limit).astype(kind)


def setup_inputs(seed: int = 0) -> dict:
    key_list = jax.random.split(jax.random.key(seed), 7)
    return {
        "activations": noise(key_list[0], (TOKENS, D), 1.0, 6.0, ((0, 8), (1, 4))),
        "cotangent": noise(key_list[1], (TOKENS, COLS), (TOKENS ** -0.5), 0.13183594, ((0, 8),)),
        "weight": noise(key_list[2], (D, COLS), D ** -0.5, 0.0625, ((0, 4),), jnp.float32),
        "stats_old": draw_stats_old(jax.random.fold_in(key_list[6], 71), 0),
        "owners": draw_owners(jax.random.fold_in(key_list[6], 71), 0),
        "next_acts": noise(key_list[5], (TOKENS, D), 1.0, 6.0, ((0, 8), (1, 4))),
    }


decay_rate = 0.9
step_rate = 0.01

def newton_root(stats):
    width = stats.shape[0]
    identity = jnp.eye(width, dtype=jnp.float32)
    norm_value = jnp.sqrt(jnp.sum(stats * stats) + 1e-06)
    matrix = stats / norm_value
    iterate = identity
    for counter in range(ITERS):
        factor = (5.0 * identity - matrix) / 4.0
        factor_low = factor.astype(jnp.bfloat16)
        iterate = jnp.dot(iterate.astype(jnp.bfloat16), factor_low, preferred_element_type=jnp.float32)
        if counter + 1 < ITERS:
            square = jnp.dot(factor_low, factor_low, preferred_element_type=jnp.float32).astype(jnp.bfloat16)
            fourth = jnp.dot(square, square, preferred_element_type=jnp.float32).astype(jnp.bfloat16)
            matrix = jnp.dot(fourth, matrix.astype(jnp.bfloat16), preferred_element_type=jnp.float32)
    return iterate * norm_value ** (-0.25)

def one_block(pair):
    grad_block, old_stats = pair
    gram = jnp.dot(grad_block, grad_block.T, preferred_element_type=jnp.float32) / BLOCK
    renewed = decay_rate * old_stats + (1.0 - decay_rate) * gram
    root_matrix = newton_root(renewed)
    update = jnp.dot(root_matrix.astype(jnp.bfloat16), grad_block, preferred_element_type=jnp.float32)
    return (renewed, update)

def reference(activations, cotangent, weight, stats_old, owners, next_acts):
    grad = jnp.dot(activations.T, cotangent, preferred_element_type=jnp.float32)
    grad_low = grad.astype(jnp.bfloat16)
    row_count = D // BLOCK
    col_blocks = COLS // BLOCK
    block_count = D // (BLOCK * N_FEAT) * col_blocks
    blocks = grad_low.reshape(row_count, BLOCK, col_blocks, BLOCK).transpose(0, 2, 1, 3).reshape(row_count * col_blocks, BLOCK, BLOCK)
    own_list = owners.reshape(-1).astype(jnp.int32)
    block_ids = jnp.arange(row_count * col_blocks, dtype=jnp.int32)
    group_id = block_ids // block_count
    same_owner = (own_list[:, None] == own_list[None, :]) & (group_id[:, None] == group_id[None, :]) & (block_ids[None, :] < block_ids[:, None])
    slot_of = lax.optimization_barrier(jnp.sum(same_owner.astype(jnp.int32), axis=1)).astype(jnp.int32)
    old_stats = stats_old[group_id, own_list, slot_of]
    renewed_all, update_all = lax.map(one_block, (blocks, old_stats))
    update = update_all.reshape(row_count, col_blocks, BLOCK, BLOCK).transpose(0, 2, 1, 3).reshape(D, COLS)
    weight_new = weight - step_rate * update
    stats_new = jnp.zeros(stats_old.shape, jnp.float32).at[group_id, own_list, slot_of].set(renewed_all)
    next_out = jnp.dot(next_acts, weight_new.astype(jnp.bfloat16), preferred_element_type=jnp.float32).astype(jnp.bfloat16)
    return (weight_new, stats_new, next_out)
```

```python
import functools

import jax
import jax.numpy as jnp
from jax import lax
from jax.experimental import pallas as pl
from jax.experimental.pallas import tpu as pltpu
from jax.sharding import PartitionSpec as P

ITERS = 6
CHUNKS = 1

decay_rate = 0.9
step_rate = 0.01
VMEM_BYTES = 48 * 1024 * 1024


def grad_kernel(width, col_blocks, per_step, order_ref, act_ref, cot_ref, out_ref):
    base = pl.program_id(0) * per_step
    for j in range(per_step):
        block = order_ref[base + j]
        rows = pl.ds(pl.multiple_of(block // col_blocks * width, width), width)
        cols = pl.ds(pl.multiple_of(block % col_blocks * width, width), width)
        out_ref[j] = lax.dot_general(
            act_ref[:, rows],
            cot_ref[:, cols],
            (((0,), (0,)), ((), ())),
            preferred_element_type=jnp.float32,
        ).astype(out_ref.dtype)


def permuted_grad(order, activations, cotangent, width):
    total = order.shape[0]
    tokens, rows = activations.shape
    cols = cotangent.shape[1]
    per_step = 4 if total % 4 == 0 else 1
    return pl.pallas_call(
        functools.partial(grad_kernel, width, cols // width, per_step),
        out_shape=jax.ShapeDtypeStruct((total, width, width), jnp.bfloat16),
        grid_spec=pltpu.PrefetchScalarGridSpec(
            num_scalar_prefetch=1,
            grid=(total // per_step,),
            in_specs=[
                pl.BlockSpec((tokens, rows), lambda i, o: (0, 0)),
                pl.BlockSpec((tokens, cols), lambda i, o: (0, 0)),
            ],
            out_specs=pl.BlockSpec((per_step, width, width), lambda i, o: (i, 0, 0)),
        ),
        compiler_params=pltpu.CompilerParams(vmem_limit_bytes=VMEM_BYTES),
        cost_estimate=pl.CostEstimate(
            flops=2 * total * width * width * tokens,
            bytes_accessed=2 * (tokens * (rows + cols) + total * width * width),
            transcendentals=0,
        ),
        name="permuted_grad",
    )(order, activations, cotangent)


def newton_kernel(slots, width, alive_ref, grad_ref, old_ref, stats_ref, update_ref, mat_ref, iter_ref):
    row = lax.broadcasted_iota(jnp.int32, (width, width), 0)
    col = lax.broadcasted_iota(jnp.int32, (width, width), 1)
    identity = jnp.where(row == col, 1.0, 0.0).astype(jnp.float32)
    dot = functools.partial(jnp.dot, preferred_element_type=jnp.float32)
    norms = []
    for k in range(slots):
        g = grad_ref[k]
        gram = (
            lax.dot_general(g, g, (((1,), (1,)), ((), ())), preferred_element_type=jnp.float32)
            / width
        )
        renewed = decay_rate * old_ref[k] + (1.0 - decay_rate) * gram
        stats_ref[k] = jnp.where(alive_ref[k] > 0, renewed, 0.0)
        norm = jnp.sqrt(jnp.sum(renewed * renewed, keepdims=True) + 1e-06)
        norms.append(norm)
        mat_ref[k] = renewed / norm

    def factors():
        return [((5.0 * identity - mat_ref[k]) / 4.0).astype(jnp.bfloat16) for k in range(slots)]

    def advance(low):
        square = [dot(low[k], low[k]).astype(jnp.bfloat16) for k in range(slots)]
        fourth = [dot(square[k], square[k]).astype(jnp.bfloat16) for k in range(slots)]
        for k in range(slots):
            mat_ref[k] = dot(fourth[k], mat_ref[k].astype(jnp.bfloat16))

    low = factors()
    for k in range(slots):
        iter_ref[k] = low[k]
    advance(low)

    @pl.loop(1, ITERS - 1)
    def _(step):
        low = factors()
        for k in range(slots):
            iter_ref[k] = dot(iter_ref[k], low[k]).astype(jnp.bfloat16)
        advance(low)

    low = factors()
    for k in range(slots):
        root = dot(iter_ref[k], low[k]) * norms[k] ** (-0.25)
        update_ref[k] = dot(root.astype(jnp.bfloat16), grad_ref[k]).astype(jnp.bfloat16)


def newton(alive, grad, old):
    slots, width, _ = grad.shape
    vmem = pl.BlockSpec(memory_space=pltpu.VMEM)
    return pl.pallas_call(
        functools.partial(newton_kernel, slots, width),
        out_shape=(
            jax.ShapeDtypeStruct((slots, width, width), jnp.float32),
            jax.ShapeDtypeStruct((slots, width, width), jnp.bfloat16),
        ),
        in_specs=[pl.BlockSpec(memory_space=pltpu.SMEM), vmem, vmem],
        out_specs=(vmem, vmem),
        scratch_shapes=[
            pltpu.VMEM((slots, width, width), jnp.float32),
            pltpu.VMEM((slots, width, width), jnp.bfloat16),
        ],
        compiler_params=pltpu.CompilerParams(vmem_limit_bytes=VMEM_BYTES),
        cost_estimate=pl.CostEstimate(
            flops=2 * slots * 23 * width**3,
            bytes_accessed=slots * width * width * 12,
            transcendentals=0,
        ),
        name="newton",
    )(alive, grad, old)


def apply_kernel(width, col_blocks, chunks, place_ref, weight_ref, acts_ref, *refs):
    gathered = refs[:chunks]
    new_ref, part_ref, acc_ref = refs[chunks:]
    r = pl.program_id(0)

    @pl.when(r == 0)
    def _():
        acc_ref[...] = jnp.zeros_like(acc_ref)

    for c in range(col_blocks):
        cols = slice(c * width, (c + 1) * width)
        which = place_ref[0, r * col_blocks + c]
        index = place_ref[1, r * col_blocks + c]
        update = gathered[0][index]
        for n in range(1, chunks):
            update = jnp.where(which == n, gathered[n][index], update)
        fresh = weight_ref[:, cols] - step_rate * update.astype(jnp.float32)
        new_ref[:, cols] = fresh
        acc_ref[:, cols] += jnp.dot(
            acts_ref[...], fresh.astype(jnp.bfloat16), preferred_element_type=jnp.float32
        )

    @pl.when(r == pl.num_programs(0) - 1)
    def _():
        part_ref[...] = acc_ref[...].astype(part_ref.dtype)


def apply_update(place, weight, acts, gathered):
    width = gathered[0].shape[-1]
    rows, cols = weight.shape
    tokens = acts.shape[0]
    return pl.pallas_call(
        functools.partial(apply_kernel, width, cols // width, len(gathered)),
        out_shape=(
            jax.ShapeDtypeStruct((rows, cols), jnp.float32),
            jax.ShapeDtypeStruct((tokens, cols), jnp.bfloat16),
        ),
        grid_spec=pltpu.PrefetchScalarGridSpec(
            num_scalar_prefetch=1,
            grid=(rows // width,),
            in_specs=[
                pl.BlockSpec((width, cols), lambda i, p: (i, 0)),
                pl.BlockSpec((tokens, width), lambda i, p: (0, i)),
            ]
            + [pl.BlockSpec(g.shape, lambda i, p: (0, 0, 0), pipeline_mode=pl.Buffered(1)) for g in gathered],
            out_specs=(
                pl.BlockSpec((width, cols), lambda i, p: (i, 0)),
                pl.BlockSpec((tokens, cols), lambda i, p: (0, 0)),
            ),
            scratch_shapes=[pltpu.VMEM((tokens, cols), jnp.float32)],
        ),
        compiler_params=pltpu.CompilerParams(vmem_limit_bytes=VMEM_BYTES),
        cost_estimate=pl.CostEstimate(
            flops=2 * rows * cols * tokens,
            bytes_accessed=8 * rows * cols + 2 * sum(g.size for g in gathered),
            transcendentals=0,
        ),
        name="apply_update",
    )(place, weight, acts, *gathered)


def body(n_dp, activations, cotangent, weight, stats_old, owners, next_acts):
    width = stats_old.shape[-1]
    slots = stats_old.shape[2]
    rows_dev, columns = weight.shape
    row_blocks = rows_dev // width
    col_blocks = columns // width
    block_count = row_blocks * col_blocks
    chunks = CHUNKS if slots % CHUNKS == 0 else 1
    per = slots // chunks
    feat_index = lax.axis_index("feat")
    data_index = lax.axis_index("dp")
    own_list = lax.dynamic_slice_in_dim(owners, feat_index * row_blocks, row_blocks, 0).reshape(
        block_count
    )
    ids = jnp.arange(block_count, dtype=jnp.int32)
    slot_of = jnp.sum(
        ((own_list[:, None] == own_list[None, :]) & (ids[None, :] < ids[:, None])).astype(jnp.int32),
        axis=1,
    )
    chunk_of = slot_of // per
    index_of = own_list * per + slot_of % per
    place = jnp.stack([chunk_of, index_of])
    flat = chunk_of * (n_dp * per) + index_of
    held = flat[None, :] == jnp.arange(n_dp * slots, dtype=jnp.int32)[:, None]
    order = jnp.sum(jnp.where(held, ids[None, :], 0), axis=1)
    taken = jnp.sum(
        ((own_list == data_index)[None, :] & (slot_of[None, :] == jnp.arange(slots)[:, None])).astype(
            jnp.int32
        ),
        axis=1,
    )
    old = stats_old[0, 0]
    sums = []
    for n in range(chunks):
        part = permuted_grad(
            order[n * n_dp * per : (n + 1) * n_dp * per], activations, cotangent, width
        )
        sums.append(lax.psum_scatter(part, "dp", scatter_dimension=0, tiled=True))
    stats_list, gathered = [], []
    for n in range(chunks):
        span = slice(n * per, (n + 1) * per)
        stats, update = newton(taken[span], sums[n], old[span])
        stats_list.append(stats)
        gathered.append(lax.all_gather(update, "dp", axis=0, tiled=True))
    weight_new, partial_next = apply_update(place, weight, next_acts, gathered)
    stats_out = stats_list[0] if chunks == 1 else jnp.concatenate(stats_list)
    next_out = lax.psum_scatter(partial_next, "feat", scatter_dimension=1, tiled=True)
    return (weight_new, stats_out[None, None], next_out)


def solution(mesh):
    placed = (
        P("dp", "feat"),
        P("dp", None),
        P("feat", None),
        P("feat", "dp", None, None, None),
        P(),
        P("dp", "feat"),
    )
    return jax.shard_map(
        functools.partial(body, mesh.shape["dp"]),
        mesh=mesh,
        in_specs=placed,
        out_specs=(P("feat", None), P("feat", "dp", None, None, None), P("dp", "feat")),
        check_vma=False,
    )
```

```python
import functools

import jax
import jax.numpy as jnp
from jax import lax
from jax.experimental import pallas as pl
from jax.experimental.pallas import tpu as pltpu
from jax.sharding import PartitionSpec as P

ITERS = 6

decay_rate = 0.9
step_rate = 0.01
VMEM_BYTES = 48 * 1024 * 1024


def spot(index, count):
    if count % 2:
        return index
    odd = lax.rem(index, 2)
    half = index // 2
    return (1 - odd) * half + odd * (count - 1 - half)


def at_spot(place, count):
    place = lax.rem(place + 2 * count, count)
    if count % 2:
        return place
    far = (2 * place) // count
    return (1 - far) * (2 * place) + far * (2 * (count - place) - 1)


def refresh_kernel(
    n, slots, width, row_ref, col_ref, act_ref, cot_ref, old_ref, stats_ref, out_ref,
    act_cut, cot_cut, first_ref, acc_ref, grad_ref, mat_ref, iter_ref, gath_ref,
    rs_send, rs_recv, ag_send, ag_recv, out_sem,
):
    me = lax.axis_index("dp")
    here = spot(me, n)
    after, before = at_spot(here + 1, n), at_spot(here - 1, n)
    forward = (slots + 1) // 2
    sign = [1 if k < forward else -1 for k in range(slots)]
    turns = sorted(range(slots), key=lambda k: (k % forward, k))
    target = {1: after, -1: before}

    barrier = pltpu.get_barrier_semaphore()
    for peer in (before, after):
        pl.semaphore_signal(
            barrier, inc=1, device_id={"dp": peer}, device_id_type=pl.DeviceIdType.MESH
        )

    for r in range(act_cut.shape[0]):
        act_cut[r] = act_ref[:, r * width : (r + 1) * width]
    for c in range(cot_cut.shape[0]):
        cot_cut[c] = cot_ref[:, c * width : (c + 1) * width]

    def term(place, k):
        index = at_spot(place, n) * slots + k
        return lax.dot_general(
            act_cut[row_ref[index]],
            cot_cut[col_ref[index]],
            (((0,), (0,)), ((), ())),
            preferred_element_type=jnp.float32,
        )

    def sum_copy(k, step, first=False):
        return pltpu.make_async_remote_copy(
            src_ref=first_ref.at[k] if first else acc_ref.at[k, step - 1],
            dst_ref=acc_ref.at[k, step],
            send_sem=rs_send.at[k, step],
            recv_sem=rs_recv.at[k, step],
            device_id={"dp": target[sign[k]]},
            device_id_type=pl.DeviceIdType.MESH,
        )

    def gather_copy(k, step, owner):
        return pltpu.make_async_remote_copy(
            src_ref=gath_ref.at[owner, k],
            dst_ref=gath_ref.at[owner, k],
            send_sem=ag_send.at[k, step],
            recv_sem=ag_recv.at[k, step],
            device_id={"dp": target[sign[k]]},
            device_id_type=pl.DeviceIdType.MESH,
        )

    def out_copy(k, step, owner):
        return pltpu.make_async_copy(
            gath_ref.at[owner, k], out_ref.at[owner, k], out_sem.at[k, step]
        )

    for k in turns:
        first_ref[k] = term(here - sign[k], k).astype(jnp.bfloat16)
    pl.semaphore_wait(barrier, 2)
    for k in turns:
        sum_copy(k, 0, True).start()

    def pass_on(step, _):
        for k in turns:
            own = term(here - sign[k] * (2 + step), k)
            sum_copy(k, step, True).wait_recv()
            acc_ref[k, step] = (acc_ref[k, step].astype(jnp.float32) + own).astype(jnp.bfloat16)
            sum_copy(k, step + 1).start()
        return 0

    lax.fori_loop(0, n - 2, pass_on, 0)
    for k in turns:
        own = term(here, k)
        sum_copy(k, n - 2, True).wait_recv()
        grad_ref[k] = (acc_ref[k, n - 2].astype(jnp.float32) + own).astype(jnp.bfloat16)

    row = lax.broadcasted_iota(jnp.int32, (width, width), 0)
    col = lax.broadcasted_iota(jnp.int32, (width, width), 1)
    identity = jnp.where(row == col, 1.0, 0.0).astype(jnp.float32)
    dot = functools.partial(jnp.dot, preferred_element_type=jnp.float32)
    norms = []
    for k in range(slots):
        g = grad_ref[k]
        gram = (
            lax.dot_general(g, g, (((1,), (1,)), ((), ())), preferred_element_type=jnp.float32)
            / width
        )
        renewed = decay_rate * old_ref[k] + (1.0 - decay_rate) * gram
        stats_ref[k] = renewed
        norm = jnp.sqrt(jnp.sum(renewed * renewed, keepdims=True) + 1e-06)
        norms.append(norm)
        mat_ref[k] = renewed / norm

    def factors():
        return [((5.0 * identity - mat_ref[k]) / 4.0).astype(jnp.bfloat16) for k in range(slots)]

    def advance(low):
        square = [dot(low[k], low[k]).astype(jnp.bfloat16) for k in range(slots)]
        fourth = [dot(square[k], square[k]).astype(jnp.bfloat16) for k in range(slots)]
        for k in range(slots):
            mat_ref[k] = dot(fourth[k], mat_ref[k].astype(jnp.bfloat16))

    low = factors()
    for k in range(slots):
        iter_ref[k] = low[k]
    advance(low)

    def newton_step(step, _):
        low = factors()
        for k in range(slots):
            iter_ref[k] = dot(iter_ref[k], low[k]).astype(jnp.bfloat16)
        advance(low)
        return 0

    lax.fori_loop(1, ITERS - 1, newton_step, 0)
    low = factors()
    for k in turns:
        root = dot(iter_ref[k], low[k]) * norms[k] ** (-0.25)
        gath_ref[me, k] = dot(root.astype(jnp.bfloat16), grad_ref[k]).astype(jnp.bfloat16)
        gather_copy(k, 0, me).start()
        out_copy(k, n - 1, me).start()

    def relay(step, _):
        for k in turns:
            owner = at_spot(here - sign[k] * (1 + step), n)
            gather_copy(k, step, owner).wait_recv()
            gather_copy(k, step + 1, owner).start()
            out_copy(k, step, owner).start()
        return 0

    lax.fori_loop(0, n - 2, relay, 0)
    for k in turns:
        owner = at_spot(here - sign[k] * (n - 1), n)
        gather_copy(k, n - 2, owner).wait_recv()
        out_copy(k, n - 2, owner).start()

    def finish(step, _):
        for k in turns:
            sum_copy(k, step, True).wait_send()
            gather_copy(k, step, me).wait_send()
            out_copy(k, step, me).wait()
        return 0

    lax.fori_loop(0, n - 1, finish, 0)
    for k in turns:
        out_copy(k, n - 1, me).wait()


def refresh(n, row_of, col_of, activations, cotangent, old):
    slots, width, _ = old.shape
    tokens = activations.shape[0]
    vmem = pl.BlockSpec(memory_space=pltpu.VMEM)
    smem = pl.BlockSpec(memory_space=pltpu.SMEM)
    dma = pltpu.SemaphoreType.DMA
    low = jnp.bfloat16
    return pl.pallas_call(
        functools.partial(refresh_kernel, n, slots, width),
        out_shape=(
            jax.ShapeDtypeStruct((slots, width, width), jnp.float32),
            jax.ShapeDtypeStruct((n, slots, width, width), low),
        ),
        in_specs=[smem, smem, vmem, vmem, vmem],
        out_specs=(vmem, pl.BlockSpec(memory_space=pl.ANY)),
        scratch_shapes=[
            pltpu.VMEM((activations.shape[1] // width, tokens, width), low),
            pltpu.VMEM((cotangent.shape[1] // width, tokens, width), low),
            pltpu.VMEM((slots, width, width), low),
            pltpu.VMEM((slots, n - 1, width, width), low),
            pltpu.VMEM((slots, width, width), low),
            pltpu.VMEM((slots, width, width), jnp.float32),
            pltpu.VMEM((slots, width, width), low),
            pltpu.VMEM((n, slots, width, width), low),
            dma((slots, n - 1)),
            dma((slots, n - 1)),
            dma((slots, n - 1)),
            dma((slots, n - 1)),
            dma((slots, n)),
        ],
        compiler_params=pltpu.CompilerParams(
            vmem_limit_bytes=VMEM_BYTES, collective_id=0, has_side_effects=True
        ),
        cost_estimate=pl.CostEstimate(
            flops=2 * slots * 31 * width**3, bytes_accessed=100_000_000, transcendentals=0
        ),
        name="refresh",
    )(row_of, col_of, activations, cotangent, old)


def total_kernel(n, part_ref, out_ref, held_ref, send_sem, recv_sem):
    me = lax.axis_index("feat")
    barrier = pltpu.get_barrier_semaphore()
    for d in range(1, n):
        pl.semaphore_signal(
            barrier,
            inc=1,
            device_id={"feat": lax.rem(me + d, n)},
            device_id_type=pl.DeviceIdType.MESH,
        )
    pl.semaphore_wait(barrier, n - 1)
    copies = []
    for d in range(1, n):
        peer = lax.rem(me + d, n)
        copy = pltpu.make_async_remote_copy(
            src_ref=part_ref.at[peer],
            dst_ref=held_ref.at[d - 1],
            send_sem=send_sem.at[d - 1],
            recv_sem=recv_sem.at[d - 1],
            device_id={"feat": peer},
            device_id_type=pl.DeviceIdType.MESH,
        )
        copy.start()
        copies.append(copy)
    total = part_ref[me].astype(jnp.float32)
    for d in range(1, n):
        copies[d - 1].wait_recv()
        total = total + held_ref[d - 1].astype(jnp.float32)
    out_ref[...] = total.astype(out_ref.dtype)
    for copy in copies:
        copy.wait_send()


def total_over_feat(n, parts):
    _, tokens, cols = parts.shape
    vmem = pl.BlockSpec(memory_space=pltpu.VMEM)
    return pl.pallas_call(
        functools.partial(total_kernel, n),
        out_shape=jax.ShapeDtypeStruct((tokens, cols), parts.dtype),
        in_specs=[vmem],
        out_specs=vmem,
        scratch_shapes=[
            pltpu.VMEM((n - 1, tokens, cols), parts.dtype),
            pltpu.SemaphoreType.DMA((n - 1,)),
            pltpu.SemaphoreType.DMA((n - 1,)),
        ],
        compiler_params=pltpu.CompilerParams(collective_id=1, has_side_effects=True),
        name="total_over_feat",
    )(parts)


def apply_kernel(width, col_blocks, splits, place_ref, weight_ref, acts_ref, gath_ref, new_ref, part_ref, acc_ref):
    r = pl.program_id(0)

    @pl.when(r == 0)
    def _():
        acc_ref[...] = jnp.zeros_like(acc_ref)

    for c in range(col_blocks):
        cols = slice(c * width, (c + 1) * width)
        update = gath_ref[place_ref[r * col_blocks + c]]
        fresh = weight_ref[:, cols] - step_rate * update.astype(jnp.float32)
        new_ref[:, cols] = fresh
        acc_ref[:, cols] += jnp.dot(
            acts_ref[...], fresh.astype(jnp.bfloat16), preferred_element_type=jnp.float32
        )

    @pl.when(r == pl.num_programs(0) - 1)
    def _():
        share = acc_ref.shape[1] // splits
        for f in range(splits):
            part_ref[f] = acc_ref[:, f * share : (f + 1) * share].astype(part_ref.dtype)


def apply_update(place, weight, acts, gathered, splits):
    width = gathered.shape[-1]
    rows, cols = weight.shape
    tokens = acts.shape[0]
    share = cols // splits
    return pl.pallas_call(
        functools.partial(apply_kernel, width, cols // width, splits),
        out_shape=(
            jax.ShapeDtypeStruct((rows, cols), jnp.float32),
            jax.ShapeDtypeStruct((splits, tokens, share), jnp.bfloat16),
        ),
        grid_spec=pltpu.PrefetchScalarGridSpec(
            num_scalar_prefetch=1,
            grid=(rows // width,),
            in_specs=[
                pl.BlockSpec((width, cols), lambda i, p: (i, 0)),
                pl.BlockSpec((tokens, width), lambda i, p: (0, i)),
                pl.BlockSpec(
                    gathered.shape, lambda i, p: (0, 0, 0), pipeline_mode=pl.Buffered(1)
                ),
            ],
            out_specs=(
                pl.BlockSpec((width, cols), lambda i, p: (i, 0)),
                pl.BlockSpec((splits, tokens, share), lambda i, p: (0, 0, 0)),
            ),
            scratch_shapes=[pltpu.VMEM((tokens, cols), jnp.float32)],
        ),
        compiler_params=pltpu.CompilerParams(vmem_limit_bytes=VMEM_BYTES),
        cost_estimate=pl.CostEstimate(
            flops=2 * rows * cols * tokens,
            bytes_accessed=8 * rows * cols + 2 * gathered.size,
            transcendentals=0,
        ),
        name="apply_update",
    )(place, weight, acts, gathered)


def body(n_dp, n_feat, activations, cotangent, weight, stats_old, owners, next_acts):
    width = stats_old.shape[-1]
    slots = stats_old.shape[2]
    rows_dev, columns = weight.shape
    row_blocks = rows_dev // width
    col_blocks = columns // width
    block_count = row_blocks * col_blocks
    feat_index = lax.axis_index("feat")
    data_index = lax.axis_index("dp")
    own_list = lax.dynamic_slice_in_dim(owners, feat_index * row_blocks, row_blocks, 0).reshape(
        block_count
    )
    ids = jnp.arange(block_count, dtype=jnp.int32)
    slot_of = jnp.sum(
        ((own_list[:, None] == own_list[None, :]) & (ids[None, :] < ids[:, None])).astype(jnp.int32),
        axis=1,
    )
    place = own_list * slots + slot_of
    held = place[None, :] == jnp.arange(n_dp * slots, dtype=jnp.int32)[:, None]
    order = jnp.sum(jnp.where(held, ids[None, :], 0), axis=1)
    stats, gathered = refresh(
        n_dp, order // col_blocks, order % col_blocks, activations, cotangent, stats_old[0, 0]
    )
    if n_dp * slots != block_count:
        mine = (own_list == data_index)[None, :] & (slot_of[None, :] == jnp.arange(slots)[:, None])
        stats = jnp.where(jnp.any(mine, axis=1)[:, None, None], stats, 0.0)
    gathered = gathered.reshape(n_dp * slots, width, width)
    direct = columns % (128 * n_feat) == 0
    weight_new, parts = apply_update(
        place, weight, next_acts, gathered, n_feat if direct else 1
    )
    if direct:
        next_out = total_over_feat(n_feat, parts)
    else:
        next_out = lax.psum_scatter(parts[0], "feat", scatter_dimension=1, tiled=True)
    return (weight_new, stats[None, None], next_out)


def solution(mesh):
    placed = (
        P("dp", "feat"),
        P("dp", None),
        P("feat", None),
        P("feat", "dp", None, None, None),
        P(),
        P("dp", "feat"),
    )
    return jax.shard_map(
        functools.partial(body, mesh.shape["dp"], mesh.shape["feat"]),
        mesh=mesh,
        in_specs=placed,
        out_specs=(P("feat", None), P("feat", "dp", None, None, None), P("dp", "feat")),
        check_vma=False,
    )
```

```python
import functools

import jax
import jax.numpy as jnp
from jax import lax
from jax.experimental import pallas as pl
from jax.experimental.pallas import tpu as pltpu
from jax.sharding import PartitionSpec as P

ITERS = 6

decay_rate = 0.9
step_rate = 0.01
VMEM_BYTES = 48 * 1024 * 1024
REFRESH_BYTES = 20 * 1024 * 1024
APPLY_BYTES = 16 * 1024 * 1024
TOTAL_BYTES = 4 * 1024 * 1024


def spot(index, count):
    if count % 2:
        return index
    odd = lax.rem(index, 2)
    half = index // 2
    return (1 - odd) * half + odd * (count - 1 - half)


def at_spot(place, count):
    place = lax.rem(place + 2 * count, count)
    if count % 2:
        return place
    far = (2 * place) // count
    return (1 - far) * (2 * place) + far * (2 * (count - place) - 1)


def refresh_kernel(
    n, slots, width, row_ref, col_ref, act_ref, cot_ref, old_hbm, stats_ref, gath_ref,
    act_cut, cot_cut, old_ref, first_ref, acc_ref, grad_ref, mat_ref, iter_ref,
    rs_send, rs_recv, ag_send, ag_recv, act_sem, cot_sem, old_sem,
):
    me = lax.axis_index("dp")
    here = spot(me, n)
    after, before = at_spot(here + 1, n), at_spot(here - 1, n)
    forward = (slots + 1) // 2
    sign = [1 if k < forward else -1 for k in range(slots)]
    turns = sorted(range(slots), key=lambda k: (k % forward, k))
    target = {1: after, -1: before}

    barrier = pltpu.get_barrier_semaphore()
    for peer in (before, after):
        pl.semaphore_signal(
            barrier, inc=1, device_id={"dp": peer}, device_id_type=pl.DeviceIdType.MESH
        )

    cuts = [
        pltpu.make_async_copy(
            cot_ref.at[:, c * width : (c + 1) * width], cot_cut.at[c], cot_sem.at[c]
        )
        for c in range(cot_cut.shape[0])
    ] + [
        pltpu.make_async_copy(
            act_ref.at[:, r * width : (r + 1) * width], act_cut.at[r], act_sem.at[r]
        )
        for r in range(act_cut.shape[0])
    ]
    load_old = pltpu.make_async_copy(old_hbm, old_ref, old_sem)
    for cut in cuts:
        cut.start()
    load_old.start()

    def term(place, k):
        index = at_spot(place, n) * slots + k
        return lax.dot_general(
            act_cut[row_ref[index]],
            cot_cut[col_ref[index]],
            (((0,), (0,)), ((), ())),
            preferred_element_type=jnp.float32,
        )

    def sum_copy(k, step, first=False):
        return pltpu.make_async_remote_copy(
            src_ref=first_ref.at[k] if first else acc_ref.at[k, step - 1],
            dst_ref=acc_ref.at[k, step],
            send_sem=rs_send.at[k, step],
            recv_sem=rs_recv.at[k, step],
            device_id={"dp": target[sign[k]]},
            device_id_type=pl.DeviceIdType.MESH,
        )

    def gather_copy(k, step, owner):
        return pltpu.make_async_remote_copy(
            src_ref=gath_ref.at[owner, k],
            dst_ref=gath_ref.at[owner, k],
            send_sem=ag_send.at[k, step],
            recv_sem=ag_recv.at[k, step],
            device_id={"dp": target[sign[k]]},
            device_id_type=pl.DeviceIdType.MESH,
        )

    for cut in cuts:
        cut.wait()
    for k in turns:
        first_ref[k] = term(here - sign[k], k).astype(jnp.bfloat16)
    pl.semaphore_wait(barrier, 2)
    for k in turns:
        sum_copy(k, 0, True).start()

    def pass_on(step, _):
        for k in turns:
            own = term(here - sign[k] * (2 + step), k)
            sum_copy(k, step, True).wait_recv()
            acc_ref[k, step] = (acc_ref[k, step].astype(jnp.float32) + own).astype(jnp.bfloat16)
            sum_copy(k, step + 1).start()
        return 0

    lax.fori_loop(0, n - 2, pass_on, 0)
    for k in turns:
        own = term(here, k)
        sum_copy(k, n - 2, True).wait_recv()
        grad_ref[k] = (acc_ref[k, n - 2].astype(jnp.float32) + own).astype(jnp.bfloat16)

    load_old.wait()
    row = lax.broadcasted_iota(jnp.int32, (width, width), 0)
    col = lax.broadcasted_iota(jnp.int32, (width, width), 1)
    identity = jnp.where(row == col, 1.0, 0.0).astype(jnp.float32)
    dot = functools.partial(jnp.dot, preferred_element_type=jnp.float32)
    norms = []
    for k in range(slots):
        g = grad_ref[k]
        gram = (
            lax.dot_general(g, g, (((1,), (1,)), ((), ())), preferred_element_type=jnp.float32)
            / width
        )
        renewed = decay_rate * old_ref[k] + (1.0 - decay_rate) * gram
        stats_ref[k] = renewed
        norm = jnp.sqrt(jnp.sum(renewed * renewed, keepdims=True) + 1e-06)
        norms.append(norm)
        mat_ref[k] = renewed / norm

    def factors():
        return [((5.0 * identity - mat_ref[k]) / 4.0).astype(jnp.bfloat16) for k in range(slots)]

    def advance(low):
        square = [dot(low[k], low[k]).astype(jnp.bfloat16) for k in range(slots)]
        fourth = [dot(square[k], square[k]).astype(jnp.bfloat16) for k in range(slots)]
        for k in range(slots):
            mat_ref[k] = dot(fourth[k], mat_ref[k].astype(jnp.bfloat16))

    low = factors()
    for k in range(slots):
        iter_ref[k] = low[k]
    advance(low)

    def newton_step(step, _):
        low = factors()
        for k in range(slots):
            iter_ref[k] = dot(iter_ref[k], low[k]).astype(jnp.bfloat16)
        advance(low)
        return 0

    lax.fori_loop(1, ITERS - 1, newton_step, 0)
    low = factors()
    for k in turns:
        root = dot(iter_ref[k], low[k]) * norms[k] ** (-0.25)
        gath_ref[me, k] = dot(root.astype(jnp.bfloat16), grad_ref[k]).astype(jnp.bfloat16)
        gather_copy(k, 0, me).start()

    def relay(step, _):
        for k in turns:
            owner = at_spot(here - sign[k] * (1 + step), n)
            gather_copy(k, step, owner).wait_recv()
            gather_copy(k, step + 1, owner).start()
        return 0

    lax.fori_loop(0, n - 2, relay, 0)
    for k in turns:
        owner = at_spot(here - sign[k] * (n - 1), n)
        gather_copy(k, n - 2, owner).wait_recv()

    def finish(step, _):
        for k in turns:
            sum_copy(k, step, True).wait_send()
            gather_copy(k, step, me).wait_send()
        return 0

    lax.fori_loop(0, n - 1, finish, 0)


def refresh(n, row_of, col_of, activations, cotangent, old):
    slots, width, _ = old.shape
    tokens = activations.shape[0]
    vmem = pl.BlockSpec(memory_space=pltpu.VMEM)
    smem = pl.BlockSpec(memory_space=pltpu.SMEM)
    hbm = pl.BlockSpec(memory_space=pltpu.HBM)
    dma = pltpu.SemaphoreType.DMA
    low = jnp.bfloat16
    return pl.pallas_call(
        functools.partial(refresh_kernel, n, slots, width),
        out_shape=(
            jax.ShapeDtypeStruct((slots, width, width), jnp.float32),
            jax.ShapeDtypeStruct((n, slots, width, width), low),
        ),
        in_specs=[smem, smem, hbm, hbm, hbm],
        out_specs=(vmem, vmem),
        scratch_shapes=[
            pltpu.VMEM((activations.shape[1] // width, tokens, width), low),
            pltpu.VMEM((cotangent.shape[1] // width, tokens, width), low),
            pltpu.VMEM((slots, width, width), jnp.float32),
            pltpu.VMEM((slots, width, width), low),
            pltpu.VMEM((slots, n - 1, width, width), low),
            pltpu.VMEM((slots, width, width), low),
            pltpu.VMEM((slots, width, width), jnp.float32),
            pltpu.VMEM((slots, width, width), low),
            dma((slots, n - 1)),
            dma((slots, n - 1)),
            dma((slots, n - 1)),
            dma((slots, n - 1)),
            dma((activations.shape[1] // width,)),
            dma((cotangent.shape[1] // width,)),
            dma,
        ],
        compiler_params=pltpu.CompilerParams(
            vmem_limit_bytes=REFRESH_BYTES if n * slots <= 32 else VMEM_BYTES,
            collective_id=0,
            has_side_effects=True,
        ),
        cost_estimate=pl.CostEstimate(
            flops=2 * slots * 31 * width**3, bytes_accessed=100_000_000, transcendentals=0
        ),
        name="refresh",
    )(row_of, col_of, activations, cotangent, old)


def total_kernel(n, part_ref, out_ref, held_ref, send_sem, recv_sem):
    me = lax.axis_index("feat")
    barrier = pltpu.get_barrier_semaphore()
    for d in range(1, n):
        pl.semaphore_signal(
            barrier,
            inc=1,
            device_id={"feat": lax.rem(me + d, n)},
            device_id_type=pl.DeviceIdType.MESH,
        )
    pl.semaphore_wait(barrier, n - 1)
    copies = []
    for d in range(1, n):
        peer = lax.rem(me + d, n)
        copy = pltpu.make_async_remote_copy(
            src_ref=part_ref.at[peer],
            dst_ref=held_ref.at[d - 1],
            send_sem=send_sem.at[d - 1],
            recv_sem=recv_sem.at[d - 1],
            device_id={"feat": peer},
            device_id_type=pl.DeviceIdType.MESH,
        )
        copy.start()
        copies.append(copy)
    total = part_ref[me].astype(jnp.float32)
    for d in range(1, n):
        copies[d - 1].wait_recv()
        total = total + held_ref[d - 1].astype(jnp.float32)
    out_ref[...] = total.astype(out_ref.dtype)
    for copy in copies:
        copy.wait_send()


def total_over_feat(n, parts):
    _, tokens, cols = parts.shape
    vmem = pl.BlockSpec(memory_space=pltpu.VMEM)
    return pl.pallas_call(
        functools.partial(total_kernel, n),
        out_shape=jax.ShapeDtypeStruct((tokens, cols), parts.dtype),
        in_specs=[vmem],
        out_specs=vmem,
        scratch_shapes=[
            pltpu.VMEM((n - 1, tokens, cols), parts.dtype),
            pltpu.SemaphoreType.DMA((n - 1,)),
            pltpu.SemaphoreType.DMA((n - 1,)),
        ],
        compiler_params=pltpu.CompilerParams(
            vmem_limit_bytes=TOTAL_BYTES, collective_id=1, has_side_effects=True
        ),
        name="total_over_feat",
    )(parts)


def apply_kernel(width, col_blocks, splits, place_ref, weight_ref, acts_ref, gath_ref, new_ref, part_ref, acc_ref):
    r = pl.program_id(0)

    @pl.when(r == 0)
    def _():
        acc_ref[...] = jnp.zeros_like(acc_ref)

    for c in range(col_blocks):
        cols = slice(c * width, (c + 1) * width)
        update = gath_ref[place_ref[r * col_blocks + c]]
        fresh = weight_ref[:, cols] - step_rate * update.astype(jnp.float32)
        new_ref[:, cols] = fresh
        acc_ref[:, cols] += jnp.dot(
            acts_ref[...], fresh.astype(jnp.bfloat16), preferred_element_type=jnp.float32
        )

    @pl.when(r == pl.num_programs(0) - 1)
    def _():
        share = acc_ref.shape[1] // splits
        for f in range(splits):
            part_ref[f] = acc_ref[:, f * share : (f + 1) * share].astype(part_ref.dtype)


def apply_update(place, weight, acts, gathered, splits):
    width = gathered.shape[-1]
    rows, cols = weight.shape
    tokens = acts.shape[0]
    share = cols // splits
    return pl.pallas_call(
        functools.partial(apply_kernel, width, cols // width, splits),
        out_shape=(
            jax.ShapeDtypeStruct((rows, cols), jnp.float32),
            jax.ShapeDtypeStruct((splits, tokens, share), jnp.bfloat16),
        ),
        grid_spec=pltpu.PrefetchScalarGridSpec(
            num_scalar_prefetch=1,
            grid=(rows // width,),
            in_specs=[
                pl.BlockSpec((width, cols), lambda i, p: (i, 0)),
                pl.BlockSpec((tokens, width), lambda i, p: (0, i)),
                pl.BlockSpec(
                    gathered.shape, lambda i, p: (0, 0, 0), pipeline_mode=pl.Buffered(1)
                ),
            ],
            out_specs=(
                pl.BlockSpec((width, cols), lambda i, p: (i, 0)),
                pl.BlockSpec((splits, tokens, share), lambda i, p: (0, 0, 0)),
            ),
            scratch_shapes=[pltpu.VMEM((tokens, cols), jnp.float32)],
        ),
        compiler_params=pltpu.CompilerParams(vmem_limit_bytes=APPLY_BYTES if gathered.size <= 1 << 21 else VMEM_BYTES),
        cost_estimate=pl.CostEstimate(
            flops=2 * rows * cols * tokens,
            bytes_accessed=8 * rows * cols + 2 * gathered.size,
            transcendentals=0,
        ),
        name="apply_update",
    )(place, weight, acts, gathered)


def body(n_dp, n_feat, activations, cotangent, weight, stats_old, owners, next_acts):
    width = stats_old.shape[-1]
    slots = stats_old.shape[2]
    rows_dev, columns = weight.shape
    row_blocks = rows_dev // width
    col_blocks = columns // width
    block_count = row_blocks * col_blocks
    feat_index = lax.axis_index("feat")
    data_index = lax.axis_index("dp")
    own_list = lax.dynamic_slice_in_dim(owners, feat_index * row_blocks, row_blocks, 0).reshape(
        block_count
    )
    ids = jnp.arange(block_count, dtype=jnp.int32)
    slot_of = jnp.sum(
        ((own_list[:, None] == own_list[None, :]) & (ids[None, :] < ids[:, None])).astype(jnp.int32),
        axis=1,
    )
    place = own_list * slots + slot_of
    held = place[None, :] == jnp.arange(n_dp * slots, dtype=jnp.int32)[:, None]
    order = jnp.sum(jnp.where(held, ids[None, :], 0), axis=1)
    stats, gathered = refresh(
        n_dp, order // col_blocks, order % col_blocks, activations, cotangent, stats_old[0, 0]
    )
    if n_dp * slots != block_count:
        mine = (own_list == data_index)[None, :] & (slot_of[None, :] == jnp.arange(slots)[:, None])
        stats = jnp.where(jnp.any(mine, axis=1)[:, None, None], stats, 0.0)
    gathered = gathered.reshape(n_dp * slots, width, width)
    direct = columns % (128 * n_feat) == 0
    weight_new, parts = apply_update(
        place, weight, next_acts, gathered, n_feat if direct else 1
    )
    if direct:
        next_out = total_over_feat(n_feat, parts)
    else:
        next_out = lax.psum_scatter(parts[0], "feat", scatter_dimension=1, tiled=True)
    return (weight_new, stats[None, None], next_out)


def solution(mesh):
    placed = (
        P("dp", "feat"),
        P("dp", None),
        P("feat", None),
        P("feat", "dp", None, None, None),
        P(),
        P("dp", "feat"),
    )
    return jax.shard_map(
        functools.partial(body, mesh.shape["dp"], mesh.shape["feat"]),
        mesh=mesh,
        in_specs=placed,
        out_specs=(P("feat", None), P("feat", "dp", None, None, None), P("dp", "feat")),
        check_vma=False,
    )
```
